32 devices in a mesh: groups: 2 (over x), seq: 16 (over z, y, core).
Axes of the slice: x: 2, y: 2, z: 4, core: 2. Of those that a mesh axis runs over, the one named last changes fastest.
Arguments:
- q_rows: bfloat16 [4096, 2048], P(('groups', 'seq')), parts along dimension 0, may hold values from -6 to 6
- k_rows: bfloat16 [4096, 2048], P(('groups', 'seq')), parts along dimension 0, may hold values from -6 to 6
- v_rows: bfloat16 [4096, 2048], P(('groups', 'seq')), parts along dimension 0, may hold values from -6 to 6
- block_of: int32 [4096, 1], P(('groups', 'seq')), parts along dimension 0, may hold values from 0 to 15; in each aligned block of 128 rows (0 to 127, 128 to 255, ...) at most 12 rows name the same one
- modality: int32 [4096], P(('groups', 'seq')), parts along dimension 0, may hold values from 0 to 2
- out_gain: float32 [3, 2048], replicated, may hold values from 0.1 to 1.9
Outputs:
- mixed: bfloat16 [4096, 2048], P(('groups', 'seq')), parts along dimension 0
The draws below stay inside these ranges and needn't reach their ends.
There are 2 independent parts, one for each index of `groups`. The reference program is written for one: setup_inputs(seed, part) draws one part's arguments, and reference() takes and returns one part's arrays. A program takes and returns all parts, laid end to end along the dimension named above; an argument that names none is the same for every part. Nothing has to cross between parts.
Inputs may be any that keep to these rules, and one draw needn't show every extreme that they name: `block_of`: among the rows of one device no block is named more than 12 times, and some block is named exactly 12 times by the rows of some device.
All inputs are finite; a program needn't handle non-finite values.
Results may differ from the reference program's by a relative error of at most 0.0057.
Values may be sent and summed in bfloat16 or wider, within the bound.
No kernel may reach another device: no remote copies, remote signals or barrier semaphores. Data moves between devices by JAX's collectives and lax.ppermute only.
A program may use at most 192 MiB of HBM per device.

```python
import math
import jax
import jax.numpy as jnp
import numpy as np
from jax import lax

HEADS = 16
HEAD_DIM = 128
MODES = 3
TOK_DEV = 128
CAP = 12
TOKENS = 2048
N_SEQ = 16


def plant(entries, stream_key, least, high):
    shape = entries.shape
    place = [jax.random.randint(jax.random.fold_in(stream_key, axis), (), 0, shape[axis]) for axis in range(len(shape))]
    entries = entries.at[tuple(place)].set(least)
    longest = shape.index(max(shape))
    place[longest] = (place[longest] + 1) % shape[longest]
    return entries.at[tuple(place)].set(high)


def block_scale(stream_key, extent, shards, smallest, largest):
    level, own = 1.0, jax.random.fold_in(stream_key, 6)
    for axis_at, blocks in shards:
        draws = jnp.exp(jax.random.uniform(jax.random.fold_in(own, axis_at), (blocks,), jnp.float32, smallest / len(shards), largest / len(shards)))
        level = level * jnp.repeat(draws, extent[axis_at] // blocks).reshape([-1 if axis == axis_at else 1 for axis in range(len(extent))])
    return level


def routed_block(own_key, own, number, rows, number_of, top, reach, slope):
    sequence = jax.random.permutation(own_key, number_of)
    crowded, ordinary = portions_of(number_of, rows * top, reach, slope, True), portions_of(number_of, rows * top, reach, slope, False)
    places = jnp.arange(number_of)

    def named(lengths, turn):
        used = int((lengths > 0).sum())
        fixed = max(1, used // 4)
        moved = fixed + (places - fixed + turn * (used - fixed)) % max(1, number_of - fixed)
        return jnp.zeros((number_of,), jnp.int32).at[sequence[jnp.where(places < fixed, places, moved)]].set(jnp.asarray(lengths, jnp.int32))

    lengths = jnp.where(number % 4 == 0, named(crowded, number // 4), named(ordinary, number - number // 4 - 1))
    mixed = jax.random.permutation(jax.random.fold_in(own, 3), number_of)
    source_of, taker = mixed[0:number_of // 2 * 2:2], mixed[1:number_of // 2 * 2:2]
    room = jnp.minimum(lengths[source_of] - 1, reach - lengths[taker]) // 2
    room = jnp.where((source_of == sequence[0]) | (taker == sequence[0]) | (lengths[taker] == 0), 0, jnp.maximum(room, 0))
    moved = jax.random.randint(jax.random.fold_in(own, 4), (number_of // 2,), 0, 1 << 20) % (room + 1)
    lengths = lengths.at[source_of].add(-moved).at[taker].add(moved)
    members = jnp.searchsorted(jnp.cumsum(lengths), jnp.arange(rows * top), side="right").astype(jnp.int32)
    grid = members.reshape(top, rows).T
    grid = grid[jax.random.permutation(jax.random.fold_in(own, 1), rows)]
    turn = jax.random.randint(jax.random.fold_in(own, 2), (rows, 1), 0, top)
    return jnp.take_along_axis(grid, (jnp.arange(top)[None, :] + turn) % top, axis=1)


def portions_of(count, total, reach, skew, full):
    weights = [(1 << 20) // math.isqrt(standing ** skew) + 1 for standing in range(1, count + 1)]
    largest = reach if full else min(reach, max(-(-total // count), total * weights[0] // sum(weights)))
    least = 1 if total - largest >= count - 1 else 0
    counts, rest = [largest] + [least] * (count - 1), total - largest - least * (count - 1)
    while rest > 0:
        candidates = [i for i in range(1, count) if counts[i] < largest] or [i for i in range(1, count) if counts[i] < reach]
        whole, remaining = sum([weights[i] for i in candidates]), rest
        for i in candidates:
            extra = min(reach - counts[i], max(1, remaining * weights[i] // whole), rest)
            counts[i] = counts[i] + extra
            rest = rest - extra
    return np.array(counts)


def bell_draw(rng, extent, width, reach, pieces=(), kind=jnp.bfloat16):
    level = block_scale(rng, extent, pieces, -0.22, 0.18) if pieces else 1.0
    values = jax.random.normal(rng, extent, jnp.float32) * width * level
    return jnp.minimum(jnp.maximum(values, -reach), reach).astype(kind)


def setup_inputs(seed: int = 0, part: int = 0) -> dict:
    streams_of = jax.random.split(jax.random.key(seed), 7)
    part_splits = jax.random.split(jax.random.fold_in(streams_of[6], part), 7)
    q_rows = bell_draw(part_splits[0], (TOKENS, HEADS * HEAD_DIM), 1.0, 6.0, ((0, 16),))
    k_rows = bell_draw(part_splits[1], (TOKENS, HEADS * HEAD_DIM), 1.0, 6.0, ((0, 16),))
    v_rows = bell_draw(part_splits[2], (TOKENS, HEADS * HEAD_DIM), 1.0, 6.0, ((0, 16),))
    block_of_keys = jax.random.split(jax.random.fold_in(part_splits[3], 1), TOKENS // TOK_DEV)
    block_of_turns = jax.random.permutation(jax.random.fold_in(part_splits[3], 3), TOKENS // TOK_DEV)
    block_of = jax.vmap(lambda own, number: routed_block(jax.random.fold_in(part_splits[3], 2), own, number, TOK_DEV, N_SEQ, 1, CAP, 1))(block_of_keys, block_of_turns).reshape((TOKENS, 1))
    modality = plant(jax.random.randint(part_splits[4], (TOKENS,), 0, 3), jax.random.fold_in(part_splits[4], 1), 0, 2).astype(jnp.int32)
    out_gain = jnp.clip(1.0 + 0.18 * jax.random.normal(streams_of[5], (MODES, HEADS * HEAD_DIM), jnp.float32), 0.1, 1.9)
    return dict(q_rows=q_rows, k_rows=k_rows, v_rows=v_rows, block_of=block_of, modality=modality, out_gain=out_gain)


def reference(q_rows, k_rows, v_rows, block_of, modality, out_gain):
    row_total = q_rows.shape[0]
    row_width = q_rows.shape[1]
    slot_count = N_SEQ * CAP
    target = block_of[:, 0].astype(jnp.int32)
    member = (target[:, None] == jnp.arange(N_SEQ, dtype=jnp.int32)[None, :]).astype(jnp.int32)
    slot_rank = lax.optimization_barrier(jnp.sum((jnp.cumsum(member, axis=0) - 1) * member, axis=1)).astype(jnp.int32)
    flat_slot = (target * slot_count + slot_rank).astype(jnp.int32)
    table = jnp.full((N_SEQ * slot_count,), row_total, jnp.int32)
    table = table.at[flat_slot].set(jnp.arange(row_total, dtype=jnp.int32)).reshape(N_SEQ, slot_count)
    padding = jnp.zeros((1, row_width), q_rows.dtype)
    q_padded = jnp.concatenate([q_rows, padding], axis=0)
    k_padded = jnp.concatenate([k_rows, padding], axis=0)
    v_padded = jnp.concatenate([v_rows, padding], axis=0)
    causal = jnp.arange(slot_count)[:, None] >= jnp.arange(slot_count)[None, :]

    def advance(prefix, row_ids):
        shape_three = (slot_count, HEADS, HEAD_DIM)
        queries = q_padded[row_ids].reshape(shape_three).astype(jnp.float32)
        key_rows = k_padded[row_ids].reshape(shape_three).astype(jnp.float32)
        value_rows = v_padded[row_ids].reshape(shape_three).astype(jnp.float32)
        block_sum = jnp.einsum('shd,she->hde', key_rows, value_rows)
        rounded = lax.optimization_barrier(prefix.astype(jnp.bfloat16)).astype(jnp.float32)
        carried_part = jnp.einsum('shd,hde->she', queries, rounded)
        scores = jnp.einsum('thd,shd->hts', queries, key_rows)
        weights = lax.optimization_barrier(jnp.where(causal[None], scores, 0.0).astype(jnp.bfloat16)).astype(jnp.float32)
        local_part = jnp.einsum('hts,she->the', weights, value_rows)
        combined = carried_part + local_part
        scale = lax.rsqrt(lax.optimization_barrier(jnp.mean(combined * combined, axis=-1, keepdims=True)) + 1e-06)
        normed = (combined * scale).astype(jnp.bfloat16)
        return (prefix + block_sum, normed.reshape(slot_count, row_width))
    start = jnp.zeros((HEADS, HEAD_DIM, HEAD_DIM), jnp.float32)
    final_prefix, outputs = lax.scan(advance, start, table)
    returned = outputs.reshape(N_SEQ * slot_count, row_width)[flat_slot]
    gains = out_gain[modality]
    return (returned.astype(jnp.float32) * gains).astype(jnp.bfloat16)
```

```python
import math

import jax
import jax.numpy as jnp
from jax import lax
from jax.experimental import pallas as pl
from jax.experimental.pallas import tpu as pltpu
from jax.sharding import PartitionSpec as P

HEADS = 16
HEAD_DIM = 128


def entering(part, axis, combine, identity):
    place = lax.axis_index(axis)
    gathered = lax.all_gather(part, axis)
    state = jnp.zeros_like(part) + jnp.asarray(identity, part.dtype)

    def one(lap, state):
        return combine(state, lax.dynamic_index_in_dim(gathered, lap, 0, False))

    return lax.fori_loop(0, place, one, state)


def block_state(key_rows, value_rows):
    return jnp.einsum("shd,she->hde", key_rows, value_rows, preferred_element_type=jnp.float32)


def add_states(earlier, later):
    return earlier + later


def attend(queries, row_order, key_rows, value_rows, carried):
    row_count = queries.shape[0]
    head_count = queries.shape[1]
    slot_count = key_rows.shape[0]
    group_size = math.gcd(head_count, 4)
    carried_part = jnp.einsum("rhd,hde->rhe", queries, carried, preferred_element_type=jnp.float32)
    causal = row_order[:, None] >= jnp.arange(slot_count, dtype=jnp.int32)[None, :]

    def one_group(group_id):
        query_group = lax.dynamic_slice_in_dim(queries, group_id * group_size, group_size, 1)
        key_group = lax.dynamic_slice_in_dim(key_rows, group_id * group_size, group_size, 1)
        value_group = lax.dynamic_slice_in_dim(value_rows, group_id * group_size, group_size, 1)
        scores = jnp.einsum(
            "rhd,shd->hrs", query_group, key_group, preferred_element_type=jnp.float32
        )
        weights = jnp.where(causal[None], scores, 0.0).astype(jnp.bfloat16)
        return jnp.einsum("hrs,she->rhe", weights, value_group, preferred_element_type=jnp.float32)

    pieces = lax.map(one_group, jnp.arange(head_count // group_size, dtype=jnp.int32))
    local_part = jnp.moveaxis(pieces, 0, 1).reshape(row_count, head_count, queries.shape[2])
    combined = carried_part + local_part
    scale = lax.rsqrt(jnp.mean(combined * combined, axis=-1, keepdims=True) + 1e-06)
    return (combined * scale).astype(jnp.bfloat16)


def by_blocks(q_rows, k_rows, v_rows, block_of, modality, out_gain):
    tok_count = q_rows.shape[0]
    row_width = q_rows.shape[1]
    peer_count = lax.axis_size("seq")
    capacity = max(2, 3 * tok_count // (2 * peer_count))
    slot_count = peer_count * capacity
    head_count = HEADS
    head_size = HEAD_DIM
    target = block_of[:, 0]
    member = (target[:, None] == jnp.arange(peer_count, dtype=jnp.int32)[None, :]).astype(jnp.int32)
    slot_rank = jnp.sum((jnp.cumsum(member, axis=0) - 1) * member, axis=1)
    slot_index = target * capacity + slot_rank

    def packed(row_block):
        buffer = jnp.zeros((slot_count, row_width), row_block.dtype).at[slot_index].set(row_block)
        return buffer.reshape(peer_count, capacity, row_width)

    q_send = packed(q_rows)
    k_send = packed(k_rows)
    v_send = packed(v_rows)
    q_recv, k_recv, v_recv = (
        lax.all_to_all(q_send, "seq", split_axis=0, concat_axis=0, tiled=True),
        lax.all_to_all(k_send, "seq", split_axis=0, concat_axis=0, tiled=True),
        lax.all_to_all(v_send, "seq", split_axis=0, concat_axis=0, tiled=True),
    )
    key_rows = k_recv.reshape(slot_count, head_count, head_size)
    value_rows = v_recv.reshape(slot_count, head_count, head_size)
    block_sum = block_state(key_rows, value_rows)
    prefix = entering(block_sum, "seq", add_states, jnp.zeros_like(block_sum))
    carried = prefix.astype(jnp.bfloat16)
    queries = q_recv.reshape(slot_count, head_count, head_size)
    normed = attend(queries, jnp.arange(slot_count, dtype=jnp.int32), key_rows, value_rows, carried)
    returned = lax.all_to_all(
        normed.reshape(peer_count, capacity, row_width),
        "seq",
        split_axis=0,
        concat_axis=0,
        tiled=True,
    )
    own_rows = returned.reshape(slot_count, row_width)[slot_index]
    chosen = modality[:, None]
    gains = jnp.where(
        chosen == 0,
        out_gain[0][None, :],
        jnp.where(chosen == 1, out_gain[1][None, :], out_gain[2][None, :]),
    )
    return (own_rows.astype(jnp.float32) * gains).astype(jnp.bfloat16)


def pack_kernel(q_ref, k_ref, v_ref, block_ref, out_ref):
    rows = q_ref.shape[0]
    size = out_ref.shape[2]
    tail = out_ref.shape[1] - 3 * rows
    marks = jnp.broadcast_to(block_ref[...].astype(jnp.float32), (tail, rows)).astype(out_ref.dtype)
    for head in range(out_ref.shape[0]):
        columns = pl.ds(head * size, size)
        out_ref[head, 0:rows, :] = q_ref[:, columns]
        out_ref[head, rows : 2 * rows, :] = k_ref[:, columns]
        out_ref[head, 2 * rows : 3 * rows, :] = v_ref[:, columns]
        out_ref[head, 3 * rows :, :] = marks


def head_kernel(in_ref, out_ref):
    peers, rows, size = out_ref.shape
    total = peers * rows
    marks = in_ref[:, 3 * rows, :].astype(jnp.float32)
    row_id = lax.broadcasted_iota(jnp.int32, (peers, rows), 0) * rows
    row_id = row_id + lax.broadcasted_iota(jnp.int32, (peers, rows), 1)
    key_row = marks * total + row_id.astype(jnp.float32)
    key_column = key_row.T
    step = math.gcd(peers, 4)
    for peer in range(peers):
        queries = in_ref[peer, 0:rows, :]
        place = key_column[:, peer : peer + 1]
        combined = jnp.zeros((rows, size), jnp.float32)
        for first in range(0, peers, step):
            keys = in_ref[first : first + step, rows : 2 * rows, :].reshape(step * rows, size)
            values = in_ref[first : first + step, 2 * rows : 3 * rows, :].reshape(step * rows, size)
            other = jnp.concatenate([key_row[i : i + 1, :] for i in range(first, first + step)], axis=1)
            scores = lax.dot_general(
                queries, keys, (((1,), (1,)), ((), ())), preferred_element_type=jnp.float32
            )
            weights = jnp.where(place >= other, scores, 0.0).astype(jnp.bfloat16)
            combined = combined + jnp.dot(weights, values, preferred_element_type=jnp.float32)
        scale = lax.rsqrt(jnp.mean(combined * combined, axis=-1, keepdims=True) + 1e-06)
        out_ref[peer] = (combined * scale).astype(out_ref.dtype)


def unpack_kernel(in_ref, mode_ref, gain_ref, out_ref):
    heads, rows, size = in_ref.shape
    modes = jnp.broadcast_to(mode_ref[...].astype(jnp.float32), (8, rows)).T[:, 0:1]
    for head in range(heads):
        columns = pl.ds(head * size, size)
        gains = jnp.where(
            modes == 0.0,
            gain_ref[0:1, columns],
            jnp.where(modes == 1.0, gain_ref[1:2, columns], gain_ref[2:3, columns]),
        )
        out_ref[:, columns] = (in_ref[head].astype(jnp.float32) * gains).astype(out_ref.dtype)


def by_heads(q_rows, k_rows, v_rows, block_of, modality, out_gain):
    rows = q_rows.shape[0]
    peers = lax.axis_size("seq")
    size = HEAD_DIM
    tail = 16
    tall = 3 * rows + tail
    step = math.gcd(peers, 4)
    packed = pl.pallas_call(
        pack_kernel,
        grid=(peers // step,),
        in_specs=[pl.BlockSpec((rows, step * size), lambda i: (0, i))] * 3
        + [pl.BlockSpec((1, rows), lambda i: (0, 0))],
        out_specs=pl.BlockSpec((step, tall, size), lambda i: (i, 0, 0)),
        out_shape=jax.ShapeDtypeStruct((peers, tall, size), q_rows.dtype),
    )(q_rows, k_rows, v_rows, block_of.reshape(1, rows))
    arrived = lax.all_to_all(packed, "seq", split_axis=0, concat_axis=0, tiled=True)
    normed = pl.pallas_call(
        head_kernel,
        in_specs=[pl.BlockSpec(memory_space=pltpu.VMEM)],
        out_specs=pl.BlockSpec(memory_space=pltpu.VMEM),
        out_shape=jax.ShapeDtypeStruct((peers, rows, size), q_rows.dtype),
    )(arrived)
    returned = lax.all_to_all(normed, "seq", split_axis=0, concat_axis=0, tiled=True)
    return pl.pallas_call(
        unpack_kernel,
        grid=(peers // step,),
        in_specs=[
            pl.BlockSpec((step, rows, size), lambda i: (i, 0, 0)),
            pl.BlockSpec((1, rows), lambda i: (0, 0)),
            pl.BlockSpec((out_gain.shape[0], step * size), lambda i: (0, i)),
        ],
        out_specs=pl.BlockSpec((rows, step * size), lambda i: (0, i)),
        out_shape=jax.ShapeDtypeStruct(q_rows.shape, q_rows.dtype),
    )(returned, modality.reshape(1, rows), out_gain)


def on_device(q_rows, k_rows, v_rows, block_of, modality, out_gain):
    rows = q_rows.shape[0]
    fits = lax.axis_size("seq") == HEADS and rows == HEAD_DIM
    plan = by_heads if fits else by_blocks
    return plan(q_rows, k_rows, v_rows, block_of, modality, out_gain)


def solution(mesh):
    placed = (
        P(("groups", "seq"), None),
        P(("groups", "seq"), None),
        P(("groups", "seq"), None),
        P(("groups", "seq"), None),
        P(("groups", "seq")),
        P(),
    )
    return jax.shard_map(
        on_device, mesh=mesh, in_specs=placed, out_specs=P(("groups", "seq"), None), check_vma=False
    )
```

```python
import functools
import math

import jax
import jax.numpy as jnp
from jax import lax
from jax.experimental import pallas as pl
from jax.experimental.pallas import tpu as pltpu
from jax.sharding import PartitionSpec as P

HEADS = 16
HEAD_DIM = 128
TAIL = 16
LATE = 2
TILE = 2
VMEM = pl.BlockSpec(memory_space=pltpu.VMEM)
SMEM = pl.BlockSpec(memory_space=pltpu.SMEM)


def entering(part, axis, combine, identity):
    place = lax.axis_index(axis)
    gathered = lax.all_gather(part, axis)
    state = jnp.zeros_like(part) + jnp.asarray(identity, part.dtype)

    def one(lap, state):
        return combine(state, lax.dynamic_index_in_dim(gathered, lap, 0, False))

    return lax.fori_loop(0, place, one, state)


def block_state(key_rows, value_rows):
    return jnp.einsum("shd,she->hde", key_rows, value_rows, preferred_element_type=jnp.float32)


def add_states(earlier, later):
    return earlier + later


def attend(queries, row_order, key_rows, value_rows, carried):
    row_count = queries.shape[0]
    head_count = queries.shape[1]
    slot_count = key_rows.shape[0]
    group_size = math.gcd(head_count, 4)
    carried_part = jnp.einsum("rhd,hde->rhe", queries, carried, preferred_element_type=jnp.float32)
    causal = row_order[:, None] >= jnp.arange(slot_count, dtype=jnp.int32)[None, :]

    def one_group(group_id):
        query_group = lax.dynamic_slice_in_dim(queries, group_id * group_size, group_size, 1)
        key_group = lax.dynamic_slice_in_dim(key_rows, group_id * group_size, group_size, 1)
        value_group = lax.dynamic_slice_in_dim(value_rows, group_id * group_size, group_size, 1)
        scores = jnp.einsum(
            "rhd,shd->hrs", query_group, key_group, preferred_element_type=jnp.float32
        )
        weights = jnp.where(causal[None], scores, 0.0).astype(jnp.bfloat16)
        return jnp.einsum("hrs,she->rhe", weights, value_group, preferred_element_type=jnp.float32)

    pieces = lax.map(one_group, jnp.arange(head_count // group_size, dtype=jnp.int32))
    local_part = jnp.moveaxis(pieces, 0, 1).reshape(row_count, head_count, queries.shape[2])
    combined = carried_part + local_part
    scale = lax.rsqrt(jnp.mean(combined * combined, axis=-1, keepdims=True) + 1e-06)
    return (combined * scale).astype(jnp.bfloat16)


def by_blocks(q_rows, k_rows, v_rows, block_of, modality, out_gain):
    tok_count = q_rows.shape[0]
    row_width = q_rows.shape[1]
    peer_count = lax.axis_size("seq")
    capacity = max(2, 3 * tok_count // (2 * peer_count))
    slot_count = peer_count * capacity
    head_count = HEADS
    head_size = HEAD_DIM
    target = block_of[:, 0]
    member = (target[:, None] == jnp.arange(peer_count, dtype=jnp.int32)[None, :]).astype(jnp.int32)
    slot_rank = jnp.sum((jnp.cumsum(member, axis=0) - 1) * member, axis=1)
    slot_index = target * capacity + slot_rank

    def packed(row_block):
        buffer = jnp.zeros((slot_count, row_width), row_block.dtype).at[slot_index].set(row_block)
        return buffer.reshape(peer_count, capacity, row_width)

    q_send = packed(q_rows)
    k_send = packed(k_rows)
    v_send = packed(v_rows)
    q_recv, k_recv, v_recv = (
        lax.all_to_all(q_send, "seq", split_axis=0, concat_axis=0, tiled=True),
        lax.all_to_all(k_send, "seq", split_axis=0, concat_axis=0, tiled=True),
        lax.all_to_all(v_send, "seq", split_axis=0, concat_axis=0, tiled=True),
    )
    key_rows = k_recv.reshape(slot_count, head_count, head_size)
    value_rows = v_recv.reshape(slot_count, head_count, head_size)
    block_sum = block_state(key_rows, value_rows)
    prefix = entering(block_sum, "seq", add_states, jnp.zeros_like(block_sum))
    carried = prefix.astype(jnp.bfloat16)
    queries = q_recv.reshape(slot_count, head_count, head_size)
    normed = attend(queries, jnp.arange(slot_count, dtype=jnp.int32), key_rows, value_rows, carried)
    returned = lax.all_to_all(
        normed.reshape(peer_count, capacity, row_width),
        "seq",
        split_axis=0,
        concat_axis=0,
        tiled=True,
    )
    own_rows = returned.reshape(slot_count, row_width)[slot_index]
    chosen = modality[:, None]
    gains = jnp.where(
        chosen == 0,
        out_gain[0][None, :],
        jnp.where(chosen == 1, out_gain[1][None, :], out_gain[2][None, :]),
    )
    return (own_rows.astype(jnp.float32) * gains).astype(jnp.bfloat16)


def pack_kernel(to_ref, q_ref, k_ref, v_ref, block_ref, *out_refs):
    rows = q_ref.shape[0]
    size = out_refs[0].shape[-1]
    marks = jnp.broadcast_to(block_ref[...].astype(jnp.float32), (TAIL, rows)).astype(q_ref.dtype)
    views = [out for out in out_refs]
    if len(out_refs[0].shape) == 3:
        views = [out_refs[0].at[i] for i in range(out_refs[0].shape[0])]
    for i, view in enumerate(views):
        columns = pl.ds(pl.multiple_of(to_ref[i] * size, size), size)
        view[0:rows, :] = q_ref[:, columns]
        view[rows : 2 * rows, :] = k_ref[:, columns]
        view[2 * rows : 3 * rows, :] = v_ref[:, columns]
        view[3 * rows :, :] = marks


def pack(to, whole, q_rows, k_rows, v_rows, marks):
    count = to.shape[0]
    rows = q_rows.shape[0]
    one = (3 * rows + TAIL, HEAD_DIM)
    shapes = [(count,) + one] if whole else [one] * count
    out = pl.pallas_call(
        pack_kernel,
        in_specs=[SMEM] + [VMEM] * 4,
        out_specs=[VMEM] * len(shapes),
        out_shape=[jax.ShapeDtypeStruct(shape, q_rows.dtype) for shape in shapes],
        compiler_params=pltpu.CompilerParams(vmem_limit_bytes=8 << 20),
        cost_estimate=pl.CostEstimate(flops=1 << 20, bytes_accessed=count << 18, transcendentals=0),
    )(to, q_rows, k_rows, v_rows, marks)
    return out[0] if whole else out


def load_chunks(first, chunks, rows, from_ref, q_ref, k_ref, v_ref, key_ref, column_ref):
    total = rows * from_ref.shape[0]
    size = q_ref.shape[1]
    for i, chunk in enumerate(chunks):
        at = (first + i) * rows
        q_ref[at : at + rows, :] = chunk[0:rows, :]
        k_ref[at : at + rows, :] = chunk[rows : 2 * rows, :]
        v_ref[at : at + rows, :] = chunk[2 * rows : 3 * rows, :]
        marks = chunk[3 * rows : 3 * rows + TAIL, :].astype(jnp.float32)[0:1, :]
        row_id = lax.broadcasted_iota(jnp.int32, (1, rows), 1) + from_ref[first + i] * rows
        key_ref[first + i : first + i + 1, :] = marks * total + row_id.astype(jnp.float32)
    columns = key_ref[...].T
    for i in range(first, first + len(chunks)):
        column_ref[i * rows : (i + 1) * rows, :] = jnp.broadcast_to(columns[:, i : i + 1], (rows, size))


def attend_tiles(queries, chunks, rows, start, q_ref, k_ref, v_ref, key_ref, column_ref):
    low, high = queries
    total = start
    query = q_ref[low:high, :]
    for first in range(chunks[0], chunks[1], TILE):
        last = min(first + TILE, chunks[1])
        keys = k_ref[first * rows : last * rows, :]
        values = v_ref[first * rows : last * rows, :]
        scores = lax.dot_general(
            query, keys, (((1,), (1,)), ((), ())), preferred_element_type=jnp.float32
        )
        column = column_ref[low:high, 0:rows]
        weights = jnp.concatenate(
            [
                jnp.where(
                    column >= key_ref[i : i + 1, :],
                    scores[:, (i - first) * rows : (i - first + 1) * rows],
                    0.0,
                ).astype(jnp.bfloat16)
                for i in range(first, last)
            ],
            axis=1,
        )
        part = jnp.dot(weights, values, preferred_element_type=jnp.float32)
        total = part if total is None else total + part
    return total


def early_kernel(far, from_ref, near_ref, *refs):
    far_refs, (sum_ref, *scratch) = refs[:far], refs[far:]
    near = near_ref.shape[0]
    rows = sum_ref.shape[0] // (near + far)
    chunks = [near_ref.at[i] for i in range(near)] + list(far_refs)
    load_chunks(0, chunks, rows, from_ref, *scratch)
    sum_ref[...] = attend_tiles((0, (near + far) * rows), (0, near + far), rows, None, *scratch)


def late_kernel(far, from_ref, sum_ref, near_ref, *refs):
    far_refs, (out_ref, *scratch) = refs[:far], refs[far:]
    near = near_ref.shape[0]
    peers, rows, _ = out_ref.shape
    chunks = [near_ref.at[i] for i in range(near)] + list(far_refs)
    load_chunks(0, chunks, rows, from_ref, *scratch)
    early = peers - LATE
    for low, high, start, keys in (
        (0, early, sum_ref[...], (early, peers)),
        (early, peers, None, (0, peers)),
    ):
        combined = attend_tiles((low * rows, high * rows), keys, rows, start, *scratch)
        scale = lax.rsqrt(jnp.mean(combined * combined, axis=-1, keepdims=True) + 1e-06)
        normed = (combined * scale).astype(out_ref.dtype)
        for i in range(low, high):
            out_ref[from_ref[i]] = normed[(i - low) * rows : (i - low + 1) * rows, :]


def attention_scratch(peers, rows):
    return [pltpu.VMEM((peers * rows, HEAD_DIM), jnp.bfloat16)] * 3 + [
        pltpu.VMEM((peers, rows), jnp.float32),
        pltpu.VMEM((peers * rows, HEAD_DIM), jnp.float32),
    ]


def unpack_kernel(in_ref, mode_ref, gain_ref, out_ref):
    heads, rows, size = in_ref.shape
    modes = jnp.broadcast_to(mode_ref[...].astype(jnp.float32), (8, rows)).T[:, 0:1]
    modes = jnp.broadcast_to(modes, (rows, size))
    for head in range(heads):
        columns = pl.ds(head * size, size)
        gains = jnp.where(
            modes == 0.0,
            gain_ref[0:1, columns],
            jnp.where(modes == 1.0, gain_ref[1:2, columns], gain_ref[2:3, columns]),
        )
        out_ref[:, columns] = (in_ref[head].astype(jnp.float32) * gains).astype(out_ref.dtype)


def by_heads(q_rows, k_rows, v_rows, block_of, modality, out_gain):
    rows = q_rows.shape[0]
    peers = lax.axis_size("seq")
    half = peers // 2
    me = lax.axis_index("seq")
    base = (me // half) * half
    marks = block_of.reshape(1, rows)
    far_bits = list(range(half, peers))
    sources = jnp.concatenate(
        [base + jnp.arange(half, dtype=jnp.int32), me ^ jnp.array(far_bits, dtype=jnp.int32)]
    ).astype(jnp.int32)
    sent = pack(sources[half : half + 2], False, q_rows, k_rows, v_rows, marks)
    sent = sent + pack(sources[half + 2 :], False, q_rows, k_rows, v_rows, marks)
    near_sent = pack(sources[:half], True, q_rows, k_rows, v_rows, marks)
    far = []
    for bit, chunk in zip(far_bits, sent):
        far.append(lax.ppermute(chunk, "seq", [(i, i ^ bit) for i in range(peers)]))
    near = lax.all_to_all(
        near_sent,
        "seq",
        split_axis=0,
        concat_axis=0,
        tiled=True,
        axis_index_groups=[list(range(half)), list(range(half, peers))],
    )
    early = peers - LATE
    limit = pltpu.CompilerParams(vmem_limit_bytes=24 << 20)
    flops = 4 * rows * rows * HEAD_DIM
    partial_sum = pl.pallas_call(
        functools.partial(early_kernel, early - half),
        in_specs=[SMEM] + [VMEM] * (1 + early - half),
        out_specs=VMEM,
        out_shape=jax.ShapeDtypeStruct((early * rows, HEAD_DIM), jnp.float32),
        scratch_shapes=attention_scratch(peers, rows),
        compiler_params=limit,
        cost_estimate=pl.CostEstimate(
            flops=flops * early * early, bytes_accessed=1 << 20, transcendentals=0
        ),
    )(sources, near, *far[: early - half])
    normed = pl.pallas_call(
        functools.partial(late_kernel, half),
        in_specs=[SMEM] + [VMEM] * (2 + half),
        out_specs=VMEM,
        out_shape=jax.ShapeDtypeStruct((peers, rows, HEAD_DIM), q_rows.dtype),
        scratch_shapes=attention_scratch(peers, rows),
        compiler_params=limit,
        cost_estimate=pl.CostEstimate(
            flops=flops * (peers * peers - early * early), bytes_accessed=1 << 20, transcendentals=0
        ),
    )(sources, partial_sum, near, *far)
    returned = lax.all_to_all(normed, "seq", split_axis=0, concat_axis=0, tiled=True)
    return pl.pallas_call(
        unpack_kernel,
        in_specs=[VMEM] * 3,
        out_specs=VMEM,
        out_shape=jax.ShapeDtypeStruct(q_rows.shape, q_rows.dtype),
        compiler_params=pltpu.CompilerParams(vmem_limit_bytes=8 << 20),
    )(returned, modality.reshape(1, rows), out_gain)


def fits_heads(peers, rows):
    return peers == HEADS and rows == HEAD_DIM and peers >= 8 and peers & (peers - 1) == 0


def on_device(q_rows, k_rows, v_rows, block_of, modality, out_gain):
    fits = fits_heads(lax.axis_size("seq"), q_rows.shape[0])
    plan = by_heads if fits else by_blocks
    return plan(q_rows, k_rows, v_rows, block_of, modality, out_gain)


def solution(mesh):
    placed = (
        P(("groups", "seq"), None),
        P(("groups", "seq"), None),
        P(("groups", "seq"), None),
        P(("groups", "seq"), None),
        P(("groups", "seq")),
        P(),
    )
    return jax.shard_map(
        on_device, mesh=mesh, in_specs=placed, out_specs=P(("groups", "seq"), None), check_vma=False
    )
```

```python
import functools
import math

import jax
import jax.numpy as jnp
from jax import lax
from jax.experimental import pallas as pl
from jax.experimental.pallas import tpu as pltpu
from jax.sharding import PartitionSpec as P

HEADS = 16
HEAD_DIM = 128
CORES = 2
TAIL = 8
TILE = 2
FIRST = 2
VMEM = pl.BlockSpec(memory_space=pltpu.VMEM)
HBM = pl.BlockSpec(memory_space=pltpu.HBM)


def entering(part, axis, combine, identity):
    place = lax.axis_index(axis)
    gathered = lax.all_gather(part, axis)
    state = jnp.zeros_like(part) + jnp.asarray(identity, part.dtype)

    def one(lap, state):
        return combine(state, lax.dynamic_index_in_dim(gathered, lap, 0, False))

    return lax.fori_loop(0, place, one, state)


def block_state(key_rows, value_rows):
    return jnp.einsum("shd,she->hde", key_rows, value_rows, preferred_element_type=jnp.float32)


def add_states(earlier, later):
    return earlier + later


def attend(queries, row_order, key_rows, value_rows, carried):
    row_count = queries.shape[0]
    head_count = queries.shape[1]
    slot_count = key_rows.shape[0]
    group_size = math.gcd(head_count, 4)
    carried_part = jnp.einsum("rhd,hde->rhe", queries, carried, preferred_element_type=jnp.float32)
    causal = row_order[:, None] >= jnp.arange(slot_count, dtype=jnp.int32)[None, :]

    def one_group(group_id):
        query_group = lax.dynamic_slice_in_dim(queries, group_id * group_size, group_size, 1)
        key_group = lax.dynamic_slice_in_dim(key_rows, group_id * group_size, group_size, 1)
        value_group = lax.dynamic_slice_in_dim(value_rows, group_id * group_size, group_size, 1)
        scores = jnp.einsum(
            "rhd,shd->hrs", query_group, key_group, preferred_element_type=jnp.float32
        )
        weights = jnp.where(causal[None], scores, 0.0).astype(jnp.bfloat16)
        return jnp.einsum("hrs,she->rhe", weights, value_group, preferred_element_type=jnp.float32)

    pieces = lax.map(one_group, jnp.arange(head_count // group_size, dtype=jnp.int32))
    local_part = jnp.moveaxis(pieces, 0, 1).reshape(row_count, head_count, queries.shape[2])
    combined = carried_part + local_part
    scale = lax.rsqrt(jnp.mean(combined * combined, axis=-1, keepdims=True) + 1e-06)
    return (combined * scale).astype(jnp.bfloat16)


def by_blocks(q_rows, k_rows, v_rows, block_of, modality, out_gain):
    tok_count = q_rows.shape[0]
    row_width = q_rows.shape[1]
    peer_count = lax.axis_size("seq")
    capacity = max(2, 3 * tok_count // (2 * peer_count))
    slot_count = peer_count * capacity
    head_count = HEADS
    head_size = HEAD_DIM
    target = block_of[:, 0]
    member = (target[:, None] == jnp.arange(peer_count, dtype=jnp.int32)[None, :]).astype(jnp.int32)
    slot_rank = jnp.sum((jnp.cumsum(member, axis=0) - 1) * member, axis=1)
    slot_index = target * capacity + slot_rank

    def packed(row_block):
        buffer = jnp.zeros((slot_count, row_width), row_block.dtype).at[slot_index].set(row_block)
        return buffer.reshape(peer_count, capacity, row_width)

    q_send = packed(q_rows)
    k_send = packed(k_rows)
    v_send = packed(v_rows)
    q_recv, k_recv, v_recv = (
        lax.all_to_all(q_send, "seq", split_axis=0, concat_axis=0, tiled=True),
        lax.all_to_all(k_send, "seq", split_axis=0, concat_axis=0, tiled=True),
        lax.all_to_all(v_send, "seq", split_axis=0, concat_axis=0, tiled=True),
    )
    key_rows = k_recv.reshape(slot_count, head_count, head_size)
    value_rows = v_recv.reshape(slot_count, head_count, head_size)
    block_sum = block_state(key_rows, value_rows)
    prefix = entering(block_sum, "seq", add_states, jnp.zeros_like(block_sum))
    carried = prefix.astype(jnp.bfloat16)
    queries = q_recv.reshape(slot_count, head_count, head_size)
    normed = attend(queries, jnp.arange(slot_count, dtype=jnp.int32), key_rows, value_rows, carried)
    returned = lax.all_to_all(
        normed.reshape(peer_count, capacity, row_width),
        "seq",
        split_axis=0,
        concat_axis=0,
        tiled=True,
    )
    own_rows = returned.reshape(slot_count, row_width)[slot_index]
    chosen = modality[:, None]
    gains = jnp.where(
        chosen == 0,
        out_gain[0][None, :],
        jnp.where(chosen == 1, out_gain[1][None, :], out_gain[2][None, :]),
    )
    return (own_rows.astype(jnp.float32) * gains).astype(jnp.bfloat16)


def pack_kernel(bits, q_ref, k_ref, v_ref, block_ref, mode_ref, *refs):
    *out_refs, note_ref, sems = refs
    rows = q_ref.shape[0]
    width = out_refs[0].shape[1]
    chip = lax.axis_index("seq") // CORES
    copies = [
        pltpu.make_async_copy(block_ref, note_ref.at[pl.ds(0, 1), :], sems.at[0]),
        pltpu.make_async_copy(mode_ref, note_ref.at[pl.ds(8, 1), :], sems.at[1]),
    ]
    for bit, out_ref in zip(bits, out_refs):
        columns = pl.ds(pl.multiple_of((chip ^ bit) * width, width), width)
        for part, ref in enumerate((q_ref, k_ref, v_ref)):
            place = out_ref.at[pl.ds(part * rows, rows), :]
            copies.append(pltpu.make_async_copy(ref.at[:, columns], place, sems.at[len(copies)]))
    for copy in copies:
        copy.start()
    for copy in copies:
        copy.wait()
    notes = jnp.concatenate([note_ref[0:1, :], note_ref[8:9, :]], axis=1).astype(jnp.float32)
    notes = jnp.broadcast_to(notes, (TAIL, 2 * rows)).astype(out_refs[0].dtype)
    for out_ref in out_refs:
        out_ref[3 * rows :, :] = notes


def pack(bits, q_rows, k_rows, v_rows, block_line, mode_line):
    count = len(bits)
    rows = q_rows.shape[0]
    shape = jax.ShapeDtypeStruct((3 * rows + TAIL, CORES * HEAD_DIM), q_rows.dtype)
    operands = [
        pltpu.with_memory_space_constraint(x, pltpu.HBM)
        for x in (q_rows, k_rows, v_rows, block_line, mode_line)
    ]
    return pl.pallas_call(
        functools.partial(pack_kernel, bits),
        in_specs=[HBM] * len(operands),
        out_specs=[VMEM] * count,
        out_shape=[shape] * count,
        scratch_shapes=[
            pltpu.VMEM((16, rows), jnp.int32),
            pltpu.SemaphoreType.DMA((3 * count + 2,)),
        ],
        compiler_params=pltpu.CompilerParams(vmem_limit_bytes=8 << 20),
        cost_estimate=pl.CostEstimate(flops=1 << 20, bytes_accessed=count << 18, transcendentals=0),
    )(*operands)


def laid_shapes(chips, rows):
    queries = (CORES, chips * rows, HEAD_DIM)
    keys = (CORES, CORES * chips * rows, HEAD_DIM)
    lines = -(-CORES * chips // 8) * 8
    return [
        (queries, jnp.bfloat16),
        (keys, jnp.bfloat16),
        (keys, jnp.bfloat16),
        ((lines, rows), jnp.float32),
        (queries[1:], jnp.float32),
        (queries, jnp.float32),
    ]


def lay(bits, direct, passed, gain_ref, q_ref, k_ref, v_ref, key_ref, column_ref, scale_ref):
    size = q_ref.shape[2]
    rows = q_ref.shape[1] // len(bits)
    total = HEADS * rows
    me = lax.axis_index("seq")
    heads = [slice(head * size, (head + 1) * size) for head in range(CORES)]
    modes = []
    for i, bit in enumerate(bits):
        for core, chunk in enumerate((direct[i], passed[i])):
            line = CORES * i + core
            at = slice(line * rows, (line + 1) * rows)
            for head, lanes in enumerate(heads):
                k_ref[head, at, :] = chunk[rows : 2 * rows, lanes]
                v_ref[head, at, :] = chunk[2 * rows : 3 * rows, lanes]
            notes = chunk[3 * rows : 3 * rows + TAIL, :].astype(jnp.float32)
            source = me ^ (CORES * bit + core)
            row_id = lax.broadcasted_iota(jnp.int32, (1, rows), 1) + source * rows
            key_ref[line : line + 1, :] = notes[0:1, 0:rows] * total + row_id.astype(jnp.float32)
            if core == 0:
                modes.append(notes[0:1, rows : 2 * rows])
        for head, lanes in enumerate(heads):
            q_ref[head, i * rows : (i + 1) * rows, :] = direct[i][0:rows, lanes]
    modes += [jnp.zeros((1, rows), jnp.float32)] * (-len(modes) % 8)
    columns = key_ref[...].T
    modes = jnp.concatenate(modes, axis=0).T
    for i in range(len(bits)):
        at = slice(i * rows, (i + 1) * rows)
        line = CORES * i
        column_ref[at, :] = jnp.broadcast_to(columns[:, line : line + 1], (rows, size))
        mode = jnp.broadcast_to(modes[:, i : i + 1], (rows, size))
        for head, lanes in enumerate(heads):
            scale_ref[head, at, :] = jnp.where(
                mode == 0.0,
                gain_ref[0:1, lanes],
                jnp.where(mode == 1.0, gain_ref[1:2, lanes], gain_ref[2:3, lanes]),
            )


def attend_tiles(total, query, column_ref, k_ref, v_ref, key_ref):
    rows = key_ref.shape[1]
    chunks = k_ref.shape[0] // rows
    for first in range(0, chunks, TILE):
        last = min(first + TILE, chunks)
        keys = k_ref[first * rows : last * rows, :]
        values = v_ref[first * rows : last * rows, :]
        scores = lax.dot_general(
            query, keys, (((1,), (1,)), ((), ())), preferred_element_type=jnp.float32
        )
        weights = [
            jnp.where(
                column_ref[...] >= key_ref[i : i + 1, :],
                scores[:, (i - first) * rows : (i - first + 1) * rows],
                0.0,
            ).astype(jnp.bfloat16)
            for i in range(first, last)
        ]
        part = jnp.dot(
            jnp.concatenate(weights, axis=1), values, preferred_element_type=jnp.float32
        )
        total = part if total is None else total + part
    return total


def meet(total, head, queries, keys):
    q_ref, _, _, _, column_ref, _ = queries
    _, k_ref, v_ref, key_ref, _, _ = keys
    return attend_tiles(
        total, q_ref[head], column_ref, k_ref.at[head], v_ref.at[head], key_ref
    )


def finish(combined, gains):
    scale = lax.rsqrt(jnp.mean(combined * combined, axis=-1, keepdims=True) + 1e-06)
    normed = (combined * scale).astype(jnp.bfloat16)
    return (normed.astype(jnp.float32) * gains).astype(jnp.bfloat16)


def read_gain(gain_ref, held_ref, sem):
    columns = held_ref.shape[1]
    start = (lax.axis_index("seq") // CORES) * columns
    window = pl.ds(pl.multiple_of(start, columns), columns)
    copy = pltpu.make_async_copy(gain_ref.at[:, window], held_ref, sem)
    copy.start()
    copy.wait()


def take_up(bits, gain_ref, refs, laid):
    lay(bits, refs[: len(bits)], refs[len(bits) :], gain_ref, *laid)


def stage_kernel(olds, bits, gain_ref, *refs):
    if not olds:
        *refs, held_ref, sem = refs
        read_gain(gain_ref, held_ref, sem)
        gain_ref = held_ref
    sets = [refs[7 * i : 7 * i + 7] for i in range(olds)]
    refs = refs[7 * olds :]
    chunks, refs = refs[: 2 * len(bits)], refs[2 * len(bits) :]
    sums, new_sum, laid = refs[:olds], refs[olds], refs[olds + 1 :]
    take_up(bits, gain_ref, chunks, laid)
    for head in range(CORES):
        for out_ref, (sum_ref, *old) in zip(sums, sets):
            out_ref[head] = meet(sum_ref[head], head, old, laid)
        combined = None
        for _, *old in sets:
            combined = meet(combined, head, laid, old)
        new_sum[head] = meet(combined, head, laid, laid)


def write_back(out_refs, head, mixed):
    rows, size = out_refs[0].shape[0], mixed.shape[1]
    for i, out_ref in enumerate(out_refs):
        out_ref[:, head * size : (head + 1) * size] = mixed[i * rows : (i + 1) * rows, :]


def out_kernel(counts, bits, gain_ref, *refs):
    sets = [refs[7 * i : 7 * i + 7] for i in range(len(counts))]
    refs = refs[7 * len(counts) :]
    chunks, refs = refs[: 2 * len(bits)], refs[2 * len(bits) :]
    outs, laid = refs[:-6], refs[-6:]
    take_up(bits, gain_ref, chunks, laid)
    for count, (sum_ref, *old) in zip(counts, sets):
        mine, outs = outs[:count], outs[count:]
        for head in range(CORES):
            combined = meet(sum_ref[head], head, old, laid)
            write_back(mine, head, finish(combined, old[5][head]))
    for head in range(CORES):
        combined = None
        for keys in [one[1:] for one in sets] + [laid]:
            combined = meet(combined, head, laid, keys)
        write_back(outs, head, finish(combined, laid[5][head]))


def call(kernel, gain, operands, out_shapes, scratch_shapes, pairs, rows, read=False):
    held = [((gain.shape[0], CORES * HEAD_DIM), jnp.float32)] if read else []
    shapes = out_shapes + held
    scratch = [pltpu.VMEM(*shape) for shape in scratch_shapes]
    return list(
        pl.pallas_call(
            kernel,
            in_specs=[HBM if read else VMEM] + [VMEM] * len(operands),
            out_specs=[VMEM] * len(shapes),
            out_shape=[jax.ShapeDtypeStruct(*shape) for shape in shapes],
            scratch_shapes=scratch + ([pltpu.SemaphoreType.DMA(())] if read else []),
            compiler_params=pltpu.CompilerParams(vmem_limit_bytes=24 << 20),
            cost_estimate=pl.CostEstimate(
                flops=8 * CORES * rows * rows * HEAD_DIM * pairs,
                bytes_accessed=1 << 20,
                transcendentals=0,
            ),
        )(gain, *operands)
    )


def unpack_kernel(bits, *refs):
    *in_refs, out_ref, sems = refs
    chip = lax.axis_index("seq") // CORES
    copies = []
    for i, (bit, in_ref) in enumerate(zip(bits, in_refs)):
        width = in_ref.shape[1]
        columns = pl.ds(pl.multiple_of((chip ^ bit) * width, width), width)
        copies.append(pltpu.make_async_copy(in_ref, out_ref.at[:, columns], sems.at[i]))
    for copy in copies:
        copy.start()
    for copy in copies:
        copy.wait()


def plan_of(chips):
    half = chips // 2
    far = list(range(half, chips))
    near = list(range(half // 2, half)) + list(range(1, half // 2))
    send = []
    for i, bit in enumerate(far):
        send += [bit] if i == len(far) - 1 else [bit] + near[i : i + 1]
    early = far[: len(far) // 2]
    stages = [[0, early[0], near[0]], early[1:] + near[1:], far[len(early) : -1], far[-1:]]
    return send, stages, far[len(early) :] + early + near


def by_heads(q_rows, k_rows, v_rows, block_of, modality, out_gain):
    rows = q_rows.shape[0]
    peers = lax.axis_size("seq")
    rows_in = (q_rows, k_rows, v_rows, block_of.reshape(1, rows), modality.reshape(1, rows))
    send, stages, order = plan_of(peers // CORES)

    def across(x, bit):
        return lax.ppermute(x, "seq", [(i, i ^ (CORES * bit)) for i in range(peers)])

    sent = list(pack(send[:FIRST], *rows_in))
    *more, own = pack(send[FIRST:] + [0], *rows_in)
    direct, passed = {0: own}, {}
    for bit, chunk in zip(send, sent + more):
        direct[bit] = across(chunk, bit)
    for bit in [bit for bits in stages for bit in bits]:
        passed[bit] = lax.ppermute(direct[bit], "seq", [(i, i ^ 1) for i in range(peers)])
    gain = pltpu.with_memory_space_constraint(out_gain, pltpu.HBM)
    sets, taken = [], []
    for number, bits in enumerate(stages):
        last = number == len(stages) - 1
        chunks = [direct[bit] for bit in bits] + [passed[bit] for bit in bits]
        operands = [x for one in sets for x in one] + chunks
        pairs = len(bits) * (2 * sum(len(one) for one in taken) + len(bits))
        laid = laid_shapes(len(bits), rows)
        if last:
            counts = [len(one) for one in taken]
            kernel = functools.partial(out_kernel, counts, bits)
            shapes = [((rows, CORES * HEAD_DIM), q_rows.dtype)] * (sum(counts) + len(bits))
            done = call(kernel, gain, operands, shapes, laid, pairs, rows)
        else:
            kernel = functools.partial(stage_kernel, len(sets), bits)
            shapes = [(one[0].shape, jnp.float32) for one in sets]
            shapes += [((CORES, len(bits) * rows, HEAD_DIM), jnp.float32)] + laid
            made = call(kernel, gain, operands, shapes, [], pairs, rows, not sets)
            if not sets:
                gain = made.pop()
            old = len(sets)
            sets = [[total] + one[1:] for total, one in zip(made, sets)] + [made[old:]]
        taken.append(bits)
    owners = [bit for bits in taken for bit in bits]
    done = dict(zip(owners, done))
    for bit in order:
        done[bit] = across(done[bit], bit)
    back = [done[bit] for bit in owners]
    return pl.pallas_call(
        functools.partial(unpack_kernel, owners),
        in_specs=[VMEM] * len(back),
        out_specs=HBM,
        out_shape=jax.ShapeDtypeStruct(q_rows.shape, q_rows.dtype),
        scratch_shapes=[pltpu.SemaphoreType.DMA((len(back),))],
        compiler_params=pltpu.CompilerParams(vmem_limit_bytes=8 << 20),
    )(*back)


def fits_heads(peers, rows):
    return peers == HEADS and rows == HEAD_DIM and peers >= 16 and peers & (peers - 1) == 0


def on_device(q_rows, k_rows, v_rows, block_of, modality, out_gain):
    fits = fits_heads(lax.axis_size("seq"), q_rows.shape[0])
    plan = by_heads if fits else by_blocks
    return plan(q_rows, k_rows, v_rows, block_of, modality, out_gain)


def solution(mesh):
    placed = (
        P(("groups", "seq"), None),
        P(("groups", "seq"), None),
        P(("groups", "seq"), None),
        P(("groups", "seq"), None),
        P(("groups", "seq")),
        P(),
    )
    return jax.shard_map(
        on_device, mesh=mesh, in_specs=placed, out_specs=P(("groups", "seq"), None), check_vma=False
    )
```

```python
import functools
import math

import jax
import jax.numpy as jnp
from jax import lax
from jax.experimental import pallas as pl
from jax.experimental.pallas import tpu as pltpu
from jax.sharding import PartitionSpec as P

HEADS = 16
HEAD_DIM = 128
CORES = 2
TAIL = 8
TILE = 2
FIRST = 2
VMEM = pl.BlockSpec(memory_space=pltpu.VMEM)
HBM = pl.BlockSpec(memory_space=pltpu.HBM)


def entering(part, axis, combine, identity):
    place = lax.axis_index(axis)
    gathered = lax.all_gather(part, axis)
    state = jnp.zeros_like(part) + jnp.asarray(identity, part.dtype)

    def one(lap, state):
        return combine(state, lax.dynamic_index_in_dim(gathered, lap, 0, False))

    return lax.fori_loop(0, place, one, state)


def block_state(key_rows, value_rows):
    return jnp.einsum("shd,she->hde", key_rows, value_rows, preferred_element_type=jnp.float32)


def add_states(earlier, later):
    return earlier + later


def attend(queries, row_order, key_rows, value_rows, carried):
    row_count = queries.shape[0]
    head_count = queries.shape[1]
    slot_count = key_rows.shape[0]
    group_size = math.gcd(head_count, 4)
    carried_part = jnp.einsum("rhd,hde->rhe", queries, carried, preferred_element_type=jnp.float32)
    causal = row_order[:, None] >= jnp.arange(slot_count, dtype=jnp.int32)[None, :]

    def one_group(group_id):
        query_group = lax.dynamic_slice_in_dim(queries, group_id * group_size, group_size, 1)
        key_group = lax.dynamic_slice_in_dim(key_rows, group_id * group_size, group_size, 1)
        value_group = lax.dynamic_slice_in_dim(value_rows, group_id * group_size, group_size, 1)
        scores = jnp.einsum(
            "rhd,shd->hrs", query_group, key_group, preferred_element_type=jnp.float32
        )
        weights = jnp.where(causal[None], scores, 0.0).astype(jnp.bfloat16)
        return jnp.einsum("hrs,she->rhe", weights, value_group, preferred_element_type=jnp.float32)

    pieces = lax.map(one_group, jnp.arange(head_count // group_size, dtype=jnp.int32))
    local_part = jnp.moveaxis(pieces, 0, 1).reshape(row_count, head_count, queries.shape[2])
    combined = carried_part + local_part
    scale = lax.rsqrt(jnp.mean(combined * combined, axis=-1, keepdims=True) + 1e-06)
    return (combined * scale).astype(jnp.bfloat16)


def by_blocks(q_rows, k_rows, v_rows, block_of, modality, out_gain):
    tok_count = q_rows.shape[0]
    row_width = q_rows.shape[1]
    peer_count = lax.axis_size("seq")
    capacity = max(2, 3 * tok_count // (2 * peer_count))
    slot_count = peer_count * capacity
    head_count = HEADS
    head_size = HEAD_DIM
    target = block_of[:, 0]
    member = (target[:, None] == jnp.arange(peer_count, dtype=jnp.int32)[None, :]).astype(jnp.int32)
    slot_rank = jnp.sum((jnp.cumsum(member, axis=0) - 1) * member, axis=1)
    slot_index = target * capacity + slot_rank

    def packed(row_block):
        buffer = jnp.zeros((slot_count, row_width), row_block.dtype).at[slot_index].set(row_block)
        return buffer.reshape(peer_count, capacity, row_width)

    q_send = packed(q_rows)
    k_send = packed(k_rows)
    v_send = packed(v_rows)
    q_recv, k_recv, v_recv = (
        lax.all_to_all(q_send, "seq", split_axis=0, concat_axis=0, tiled=True),
        lax.all_to_all(k_send, "seq", split_axis=0, concat_axis=0, tiled=True),
        lax.all_to_all(v_send, "seq", split_axis=0, concat_axis=0, tiled=True),
    )
    key_rows = k_recv.reshape(slot_count, head_count, head_size)
    value_rows = v_recv.reshape(slot_count, head_count, head_size)
    block_sum = block_state(key_rows, value_rows)
    prefix = entering(block_sum, "seq", add_states, jnp.zeros_like(block_sum))
    carried = prefix.astype(jnp.bfloat16)
    queries = q_recv.reshape(slot_count, head_count, head_size)
    normed = attend(queries, jnp.arange(slot_count, dtype=jnp.int32), key_rows, value_rows, carried)
    returned = lax.all_to_all(
        normed.reshape(peer_count, capacity, row_width),
        "seq",
        split_axis=0,
        concat_axis=0,
        tiled=True,
    )
    own_rows = returned.reshape(slot_count, row_width)[slot_index]
    chosen = modality[:, None]
    gains = jnp.where(
        chosen == 0,
        out_gain[0][None, :],
        jnp.where(chosen == 1, out_gain[1][None, :], out_gain[2][None, :]),
    )
    return (own_rows.astype(jnp.float32) * gains).astype(jnp.bfloat16)


def pack_kernel(jobs, q_ref, k_ref, v_ref, block_ref, mode_ref, *refs):
    *out_refs, note_ref, sems = refs
    rows = q_ref.shape[0]
    width = out_refs[0].shape[1]
    chip = lax.axis_index("seq") // CORES
    source = {"q": q_ref, "k": k_ref, "v": v_ref}
    copies = [
        pltpu.make_async_copy(block_ref, note_ref.at[pl.ds(0, 1), :], sems.at[0]),
        pltpu.make_async_copy(mode_ref, note_ref.at[pl.ds(8, 1), :], sems.at[1]),
    ]
    for (bit, parts), out_ref in zip(jobs, out_refs):
        columns = pl.ds(pl.multiple_of((chip ^ bit) * width, width), width)
        for part, name in enumerate(parts):
            place = out_ref.at[pl.ds(part * rows, rows), :]
            copies.append(
                pltpu.make_async_copy(source[name].at[:, columns], place, sems.at[len(copies)])
            )
    for copy in copies:
        copy.start()
    for copy in copies:
        copy.wait()
    notes = jnp.concatenate([note_ref[0:1, :], note_ref[8:9, :]], axis=1).astype(jnp.float32)
    notes = jnp.broadcast_to(notes, (TAIL, 2 * rows)).astype(out_refs[0].dtype)
    for (_, parts), out_ref in zip(jobs, out_refs):
        if "k" in parts:
            out_ref[len(parts) * rows :, :] = notes


def pack(jobs, q_rows, k_rows, v_rows, block_line, mode_line):
    rows = q_rows.shape[0]
    shapes = [
        jax.ShapeDtypeStruct(
            (len(parts) * rows + TAIL * ("k" in parts), CORES * HEAD_DIM), q_rows.dtype
        )
        for _, parts in jobs
    ]
    operands = [
        pltpu.with_memory_space_constraint(x, pltpu.HBM)
        for x in (q_rows, k_rows, v_rows, block_line, mode_line)
    ]
    count = sum(len(parts) for _, parts in jobs) + 2
    return pl.pallas_call(
        functools.partial(pack_kernel, jobs),
        in_specs=[HBM] * len(operands),
        out_specs=[VMEM] * len(jobs),
        out_shape=shapes,
        scratch_shapes=[pltpu.VMEM((16, rows), jnp.int32), pltpu.SemaphoreType.DMA((count,))],
        compiler_params=pltpu.CompilerParams(vmem_limit_bytes=8 << 20),
        cost_estimate=pl.CostEstimate(
            flops=1 << 20, bytes_accessed=len(jobs) << 18, transcendentals=0
        ),
    )(*operands)


def laid_shapes(chips, rows):
    queries = (CORES, chips * rows, HEAD_DIM)
    keys = (CORES, CORES * chips * rows, HEAD_DIM)
    lines = -(-CORES * chips // 8) * 8
    return [
        (queries, jnp.bfloat16),
        (keys, jnp.bfloat16),
        (keys, jnp.bfloat16),
        ((lines, rows), jnp.float32),
        (queries[1:], jnp.float32),
        (queries, jnp.float32),
    ]


def lay(bits, direct, passed, gain_ref, q_ref, k_ref, v_ref, key_ref, column_ref, scale_ref):
    size = q_ref.shape[2]
    rows = q_ref.shape[1] // len(bits)
    total = HEADS * rows
    me = lax.axis_index("seq")
    heads = [slice(head * size, (head + 1) * size) for head in range(CORES)]
    modes = []
    for i, bit in enumerate(bits):
        for core, chunk in enumerate((direct[i], passed[i])):
            line = CORES * i + core
            at = slice(line * rows, (line + 1) * rows)
            tail = chunk.shape[0] - TAIL
            for head, lanes in enumerate(heads):
                k_ref[head, at, :] = chunk[tail - 2 * rows : tail - rows, lanes]
                v_ref[head, at, :] = chunk[tail - rows : tail, lanes]
            notes = chunk[tail : tail + TAIL, :].astype(jnp.float32)
            source = me ^ (CORES * bit + core)
            row_id = lax.broadcasted_iota(jnp.int32, (1, rows), 1) + source * rows
            key_ref[line : line + 1, :] = notes[0:1, 0:rows] * total + row_id.astype(jnp.float32)
            if core == 0:
                modes.append(notes[0:1, rows : 2 * rows])
        if direct[i].shape[0] > 3 * rows:
            for head, lanes in enumerate(heads):
                q_ref[head, i * rows : (i + 1) * rows, :] = direct[i][0:rows, lanes]
    modes += [jnp.zeros((1, rows), jnp.float32)] * (-len(modes) % 8)
    columns = key_ref[...].T
    modes = jnp.concatenate(modes, axis=0).T
    for i in range(len(bits)):
        at = slice(i * rows, (i + 1) * rows)
        line = CORES * i
        column_ref[at, :] = jnp.broadcast_to(columns[:, line : line + 1], (rows, size))
        mode = jnp.broadcast_to(modes[:, i : i + 1], (rows, size))
        for head, lanes in enumerate(heads):
            scale_ref[head, at, :] = jnp.where(
                mode == 0.0,
                gain_ref[0:1, lanes],
                jnp.where(mode == 1.0, gain_ref[1:2, lanes], gain_ref[2:3, lanes]),
            )


def attend_tiles(total, query, column_ref, k_ref, v_ref, key_ref):
    rows = key_ref.shape[1]
    chunks = k_ref.shape[0] // rows
    for first in range(0, chunks, TILE):
        last = min(first + TILE, chunks)
        keys = k_ref[first * rows : last * rows, :]
        values = v_ref[first * rows : last * rows, :]
        scores = lax.dot_general(
            query, keys, (((1,), (1,)), ((), ())), preferred_element_type=jnp.float32
        )
        weights = [
            jnp.where(
                column_ref[...] >= key_ref[i : i + 1, :],
                scores[:, (i - first) * rows : (i - first + 1) * rows],
                0.0,
            ).astype(jnp.bfloat16)
            for i in range(first, last)
        ]
        part = jnp.dot(
            jnp.concatenate(weights, axis=1), values, preferred_element_type=jnp.float32
        )
        total = part if total is None else total + part
    return total


def meet(total, head, queries, keys):
    q_ref, _, _, _, column_ref, _ = queries
    _, k_ref, v_ref, key_ref, _, _ = keys
    return attend_tiles(
        total, q_ref[head], column_ref, k_ref.at[head], v_ref.at[head], key_ref
    )


def finish(combined, gains):
    scale = lax.rsqrt(jnp.mean(combined * combined, axis=-1, keepdims=True) + 1e-06)
    normed = (combined * scale).astype(jnp.bfloat16)
    return (normed.astype(jnp.float32) * gains).astype(jnp.bfloat16)


def read_gain(gain_ref, held_ref, sem):
    columns = held_ref.shape[1]
    start = (lax.axis_index("seq") // CORES) * columns
    window = pl.ds(pl.multiple_of(start, columns), columns)
    copy = pltpu.make_async_copy(gain_ref.at[:, window], held_ref, sem)
    copy.start()
    copy.wait()


def take_up(bits, gain_ref, refs, laid):
    lay(bits, refs[: len(bits)], refs[len(bits) :], gain_ref, *laid)


def stage_kernel(olds, bits, gain_ref, *refs):
    if not olds:
        *refs, held_ref, sem = refs
        read_gain(gain_ref, held_ref, sem)
        gain_ref = held_ref
    sets = [refs[7 * i : 7 * i + 7] for i in range(olds)]
    refs = refs[7 * olds :]
    chunks, refs = refs[: 2 * len(bits)], refs[2 * len(bits) :]
    sums, new_sum, laid = refs[:olds], refs[olds], refs[olds + 1 :]
    take_up(bits, gain_ref, chunks, laid)
    for head in range(CORES):
        for out_ref, (sum_ref, *old) in zip(sums, sets):
            out_ref[head] = meet(sum_ref[head], head, old, laid)
        combined = None
        for _, *old in sets:
            combined = meet(combined, head, laid, old)
        new_sum[head] = meet(combined, head, laid, laid)


def write_back(out_refs, head, mixed):
    rows, size = out_refs[0].shape[0], mixed.shape[1]
    for i, out_ref in enumerate(out_refs):
        out_ref[:, head * size : (head + 1) * size] = mixed[i * rows : (i + 1) * rows, :]


def rest_kernel(picks, olds, bits, gain_ref, *refs):
    sets = [refs[7 * i : 7 * i + 7] for i in range(olds)]
    refs = refs[7 * olds :]
    count = sum(high - low for _, low, high in picks)
    if bits:
        chunks, refs = refs[: 2 * len(bits)], refs[2 * len(bits) :]
        outs, laid = refs[:count], refs[count:]
        take_up(bits, gain_ref, chunks, laid)
    else:
        laid, outs = refs[:6], refs[6:]
    rows = outs[0].shape[0]
    _, k_ref, v_ref, key_ref, _, _ = laid
    for place, low, high in picks:
        sum_ref, q_ref, _, _, _, column_ref, scale_ref = sets[place]
        mine, outs = outs[: high - low], outs[high - low :]
        part = slice(low * rows, high * rows)
        for head in range(CORES):
            combined = attend_tiles(
                sum_ref[head, part, :],
                q_ref[head, part, :],
                column_ref.at[part, :],
                k_ref.at[head],
                v_ref.at[head],
                key_ref,
            )
            write_back(mine, head, finish(combined, scale_ref[head, part, :]))


def new_kernel(olds, query_ref, *refs):
    laid, refs = refs[:6], refs[6:]
    sets = [refs[7 * i + 1 : 7 * i + 7] for i in range(olds)]
    outs = refs[7 * olds :]
    size = laid[1].shape[2]
    for head in range(CORES):
        query = query_ref[:, head * size : (head + 1) * size]
        combined = None
        for _, k_ref, v_ref, key_ref, _, _ in sets + [laid]:
            combined = attend_tiles(
                combined, query, laid[4], k_ref.at[head], v_ref.at[head], key_ref
            )
        write_back(outs, head, finish(combined, laid[5][head]))


def call(kernel, gain, operands, out_shapes, scratch_shapes, pairs, rows, read=False):
    held = [((gain.shape[0], CORES * HEAD_DIM), jnp.float32)] if read else []
    shapes = out_shapes + held
    scratch = [pltpu.VMEM(*shape) for shape in scratch_shapes]
    return list(
        pl.pallas_call(
            kernel,
            in_specs=[HBM if read else VMEM] + [VMEM] * len(operands),
            out_specs=[VMEM] * len(shapes),
            out_shape=[jax.ShapeDtypeStruct(*shape) for shape in shapes],
            scratch_shapes=scratch + ([pltpu.SemaphoreType.DMA(())] if read else []),
            compiler_params=pltpu.CompilerParams(vmem_limit_bytes=24 << 20),
            cost_estimate=pl.CostEstimate(
                flops=8 * CORES * rows * rows * HEAD_DIM * pairs,
                bytes_accessed=1 << 20,
                transcendentals=0,
            ),
        )(gain, *operands)
    )


def unpack_kernel(bits, *refs):
    *in_refs, out_ref, sems = refs
    chip = lax.axis_index("seq") // CORES
    copies = []
    for i, (bit, in_ref) in enumerate(zip(bits, in_refs)):
        width = in_ref.shape[1]
        columns = pl.ds(pl.multiple_of((chip ^ bit) * width, width), width)
        copies.append(pltpu.make_async_copy(in_ref, out_ref.at[:, columns], sems.at[i]))
    for copy in copies:
        copy.start()
    for copy in copies:
        copy.wait()


def merged(picks):
    joined = []
    for place, low, high in picks:
        if joined and joined[-1][0] == place and joined[-1][2] == low:
            joined[-1] = (place, joined[-1][1], high)
        else:
            joined.append((place, low, high))
    return joined


def plan_of(chips):
    half = chips // 2
    far = list(range(half, chips))
    near = list(range(half // 2, half)) + list(range(1, half // 2))
    send = []
    for i, bit in enumerate(far):
        send += [bit] if i == len(far) - 1 else [bit] + near[i : i + 1]
    early = far[: len(far) // 2]
    stages = [[0, near[0], early[0]], near[1:] + early[1:], far[len(early) : -1], far[-1:]]
    alike = [bit for bit in near if bit < half // 2]
    other = [bit for bit in near if bit >= half // 2]
    return send, stages, far[len(early) : -1] + early + far[-1:] + alike + other[::-1]


def by_heads(q_rows, k_rows, v_rows, block_of, modality, out_gain):
    rows = q_rows.shape[0]
    peers = lax.axis_size("seq")
    rows_in = (q_rows, k_rows, v_rows, block_of.reshape(1, rows), modality.reshape(1, rows))
    send, stages, order = plan_of(peers // CORES)

    def across(x, bit):
        return lax.ppermute(x, "seq", [(i, i ^ (CORES * bit)) for i in range(peers)])

    last = send[-1]
    jobs = [(bit, "qkv") for bit in send[:-1]] + [(last, "kv"), (last, "q")]
    sent = list(pack(jobs[:FIRST], *rows_in))
    *more, own = pack(jobs[FIRST:] + [(0, "qkv")], *rows_in)
    direct, passed = {0: own}, {}
    for (bit, parts), chunk in zip(jobs, sent + more):
        chunk = across(chunk, bit)
        if parts == "q":
            query = chunk
        else:
            direct[bit] = chunk
    for bit in [bit for bits in stages for bit in bits]:
        passed[bit] = lax.ppermute(direct[bit], "seq", [(i, i ^ 1) for i in range(peers)])
    gain = pltpu.with_memory_space_constraint(out_gain, pltpu.HBM)
    sets, taken = [], []
    for bits in stages[:-1]:
        chunks = [direct[bit] for bit in bits] + [passed[bit] for bit in bits]
        pairs = len(bits) * (2 * sum(len(one) for one in taken) + len(bits))
        laid = laid_shapes(len(bits), rows)
        shapes = [(one[0].shape, jnp.float32) for one in sets]
        shapes += [((CORES, len(bits) * rows, HEAD_DIM), jnp.float32)] + laid
        kernel = functools.partial(stage_kernel, len(sets), bits)
        operands = [x for one in sets for x in one] + chunks
        made = call(kernel, gain, operands, shapes, [], pairs, rows, not sets)
        if not sets:
            gain = made.pop()
        old = len(sets)
        sets = [[total] + one[1:] for total, one in zip(made, sets)] + [made[old:]]
        taken.append(bits)
    flat = [x for one in sets for x in one]
    piece = ((rows, CORES * HEAD_DIM), q_rows.dtype)
    half = peers // CORES // 2
    picks, owners = {True: [], False: []}, {True: [], False: []}
    for place, bits in enumerate(taken):
        for low, bit in enumerate(bits):
            picks[bit >= half].append((place, low, low + 1))
            owners[bit >= half].append(bit)
    kernel = functools.partial(rest_kernel, merged(picks[True]), len(sets), [last])
    shapes = [piece] * len(owners[True]) + laid_shapes(1, rows)
    operands = flat + [direct[last], passed[last]]
    made = call(kernel, gain, operands, shapes, [], len(owners[True]), rows)
    count = len(owners[True])
    done, laid = dict(zip(owners[True], made)), made[count:]
    kernel = functools.partial(new_kernel, len(sets))
    done[last] = call(kernel, query, laid + flat, [piece], [], peers // CORES, rows)[0]
    kernel = functools.partial(rest_kernel, merged(picks[False]), len(sets), [])
    shapes = [piece] * len(owners[False])
    made = call(kernel, gain, flat + laid, shapes, [], len(owners[False]), rows)
    done.update(zip(owners[False], made))
    owners = list(done)
    for bit in order:
        done[bit] = across(done[bit], bit)
    back = [done[bit] for bit in owners]
    return pl.pallas_call(
        functools.partial(unpack_kernel, owners),
        in_specs=[VMEM] * len(back),
        out_specs=HBM,
        out_shape=jax.ShapeDtypeStruct(q_rows.shape, q_rows.dtype),
        scratch_shapes=[pltpu.SemaphoreType.DMA((len(back),))],
        compiler_params=pltpu.CompilerParams(vmem_limit_bytes=8 << 20),
    )(*back)


def fits_heads(peers, rows):
    return peers == HEADS and rows == HEAD_DIM and peers >= 16 and peers & (peers - 1) == 0


def on_device(q_rows, k_rows, v_rows, block_of, modality, out_gain):
    fits = fits_heads(lax.axis_size("seq"), q_rows.shape[0])
    plan = by_heads if fits else by_blocks
    return plan(q_rows, k_rows, v_rows, block_of, modality, out_gain)


def solution(mesh):
    placed = (
        P(("groups", "seq"), None),
        P(("groups", "seq"), None),
        P(("groups", "seq"), None),
        P(("groups", "seq"), None),
        P(("groups", "seq")),
        P(),
    )
    return jax.shard_map(
        on_device, mesh=mesh, in_specs=placed, out_specs=P(("groups", "seq"), None), check_vma=False
    )
```

```python
import functools
import math

import jax
import jax.numpy as jnp
from jax import lax
from jax.experimental import pallas as pl
from jax.experimental.pallas import tpu as pltpu
from jax.sharding import PartitionSpec as P

HEADS = 16
HEAD_DIM = 128
CORES = 2
TAIL = 8
TILE = 2
FIRST = 2
VMEM = pl.BlockSpec(memory_space=pltpu.VMEM)
HBM = pl.BlockSpec(memory_space=pltpu.HBM)


def entering(part, axis, combine, identity):
    place = lax.axis_index(axis)
    gathered = lax.all_gather(part, axis)
    state = jnp.zeros_like(part) + jnp.asarray(identity, part.dtype)

    def one(lap, state):
        return combine(state, lax.dynamic_index_in_dim(gathered, lap, 0, False))

    return lax.fori_loop(0, place, one, state)


def block_state(key_rows, value_rows):
    return jnp.einsum("shd,she->hde", key_rows, value_rows, preferred_element_type=jnp.float32)


def add_states(earlier, later):
    return earlier + later


def attend(queries, row_order, key_rows, value_rows, carried):
    row_count = queries.shape[0]
    head_count = queries.shape[1]
    slot_count = key_rows.shape[0]
    group_size = math.gcd(head_count, 4)
    carried_part = jnp.einsum("rhd,hde->rhe", queries, carried, preferred_element_type=jnp.float32)
    causal = row_order[:, None] >= jnp.arange(slot_count, dtype=jnp.int32)[None, :]

    def one_group(group_id):
        query_group = lax.dynamic_slice_in_dim(queries, group_id * group_size, group_size, 1)
        key_group = lax.dynamic_slice_in_dim(key_rows, group_id * group_size, group_size, 1)
        value_group = lax.dynamic_slice_in_dim(value_rows, group_id * group_size, group_size, 1)
        scores = jnp.einsum(
            "rhd,shd->hrs", query_group, key_group, preferred_element_type=jnp.float32
        )
        weights = jnp.where(causal[None], scores, 0.0).astype(jnp.bfloat16)
        return jnp.einsum("hrs,she->rhe", weights, value_group, preferred_element_type=jnp.float32)

    pieces = lax.map(one_group, jnp.arange(head_count // group_size, dtype=jnp.int32))
    local_part = jnp.moveaxis(pieces, 0, 1).reshape(row_count, head_count, queries.shape[2])
    combined = carried_part + local_part
    scale = lax.rsqrt(jnp.mean(combined * combined, axis=-1, keepdims=True) + 1e-06)
    return (combined * scale).astype(jnp.bfloat16)


def by_blocks(q_rows, k_rows, v_rows, block_of, modality, out_gain):
    tok_count = q_rows.shape[0]
    row_width = q_rows.shape[1]
    peer_count = lax.axis_size("seq")
    capacity = max(2, 3 * tok_count // (2 * peer_count))
    slot_count = peer_count * capacity
    head_count = HEADS
    head_size = HEAD_DIM
    target = block_of[:, 0]
    member = (target[:, None] == jnp.arange(peer_count, dtype=jnp.int32)[None, :]).astype(jnp.int32)
    slot_rank = jnp.sum((jnp.cumsum(member, axis=0) - 1) * member, axis=1)
    slot_index = target * capacity + slot_rank

    def packed(row_block):
        buffer = jnp.zeros((slot_count, row_width), row_block.dtype).at[slot_index].set(row_block)
        return buffer.reshape(peer_count, capacity, row_width)

    q_send = packed(q_rows)
    k_send = packed(k_rows)
    v_send = packed(v_rows)
    q_recv, k_recv, v_recv = (
        lax.all_to_all(q_send, "seq", split_axis=0, concat_axis=0, tiled=True),
        lax.all_to_all(k_send, "seq", split_axis=0, concat_axis=0, tiled=True),
        lax.all_to_all(v_send, "seq", split_axis=0, concat_axis=0, tiled=True),
    )
    key_rows = k_recv.reshape(slot_count, head_count, head_size)
    value_rows = v_recv.reshape(slot_count, head_count, head_size)
    block_sum = block_state(key_rows, value_rows)
    prefix = entering(block_sum, "seq", add_states, jnp.zeros_like(block_sum))
    carried = prefix.astype(jnp.bfloat16)
    queries = q_recv.reshape(slot_count, head_count, head_size)
    normed = attend(queries, jnp.arange(slot_count, dtype=jnp.int32), key_rows, value_rows, carried)
    returned = lax.all_to_all(
        normed.reshape(peer_count, capacity, row_width),
        "seq",
        split_axis=0,
        concat_axis=0,
        tiled=True,
    )
    own_rows = returned.reshape(slot_count, row_width)[slot_index]
    chosen = modality[:, None]
    gains = jnp.where(
        chosen == 0,
        out_gain[0][None, :],
        jnp.where(chosen == 1, out_gain[1][None, :], out_gain[2][None, :]),
    )
    return (own_rows.astype(jnp.float32) * gains).astype(jnp.bfloat16)


def pack_kernel(jobs, q_ref, k_ref, v_ref, block_ref, mode_ref, *refs):
    *out_refs, note_ref, sems = refs
    rows = q_ref.shape[0]
    width = out_refs[0].shape[1]
    chip = lax.axis_index("seq") // CORES
    source = {"q": q_ref, "k": k_ref, "v": v_ref}
    copies = [
        pltpu.make_async_copy(block_ref, note_ref.at[pl.ds(0, 1), :], sems.at[0]),
        pltpu.make_async_copy(mode_ref, note_ref.at[pl.ds(8, 1), :], sems.at[1]),
    ]
    for (bit, parts), out_ref in zip(jobs, out_refs):
        columns = pl.ds(pl.multiple_of((chip ^ bit) * width, width), width)
        for part, name in enumerate(parts):
            place = out_ref.at[pl.ds(part * rows, rows), :]
            copies.append(
                pltpu.make_async_copy(source[name].at[:, columns], place, sems.at[len(copies)])
            )
    for copy in copies:
        copy.start()
    for copy in copies:
        copy.wait()
    notes = jnp.concatenate([note_ref[0:1, :], note_ref[8:9, :]], axis=1).astype(jnp.float32)
    notes = jnp.broadcast_to(notes, (TAIL, 2 * rows)).astype(out_refs[0].dtype)
    for (_, parts), out_ref in zip(jobs, out_refs):
        if "k" in parts:
            out_ref[len(parts) * rows :, :] = notes


def pack(jobs, q_rows, k_rows, v_rows, block_line, mode_line):
    rows = q_rows.shape[0]
    shapes = [
        jax.ShapeDtypeStruct(
            (len(parts) * rows + TAIL * ("k" in parts), CORES * HEAD_DIM), q_rows.dtype
        )
        for _, parts in jobs
    ]
    operands = [
        pltpu.with_memory_space_constraint(x, pltpu.HBM)
        for x in (q_rows, k_rows, v_rows, block_line, mode_line)
    ]
    count = sum(len(parts) for _, parts in jobs) + 2
    return pl.pallas_call(
        functools.partial(pack_kernel, jobs),
        in_specs=[HBM] * len(operands),
        out_specs=[VMEM] * len(jobs),
        out_shape=shapes,
        scratch_shapes=[pltpu.VMEM((16, rows), jnp.int32), pltpu.SemaphoreType.DMA((count,))],
        compiler_params=pltpu.CompilerParams(vmem_limit_bytes=8 << 20),
        cost_estimate=pl.CostEstimate(
            flops=1 << 20, bytes_accessed=len(jobs) << 18, transcendentals=0
        ),
    )(*operands)


def laid_shapes(chips, rows):
    queries = (CORES, chips * rows, HEAD_DIM)
    keys = (CORES, CORES * chips * rows, HEAD_DIM)
    lines = -(-CORES * chips // 8) * 8
    return [
        (queries, jnp.bfloat16),
        (keys, jnp.bfloat16),
        (keys, jnp.bfloat16),
        ((lines, rows), jnp.float32),
        (queries[1:], jnp.float32),
        (queries, jnp.float32),
    ]


def lay(bits, direct, passed, gain_ref, q_ref, k_ref, v_ref, key_ref, column_ref, scale_ref):
    size = q_ref.shape[2]
    rows = q_ref.shape[1] // len(bits)
    total = HEADS * rows
    me = lax.axis_index("seq")
    heads = [slice(head * size, (head + 1) * size) for head in range(CORES)]
    modes = []
    for i, bit in enumerate(bits):
        for core, chunk in enumerate((direct[i], passed[i])):
            line = CORES * i + core
            at = slice(line * rows, (line + 1) * rows)
            tail = chunk.shape[0] - TAIL
            for head, lanes in enumerate(heads):
                k_ref[head, at, :] = chunk[tail - 2 * rows : tail - rows, lanes]
                v_ref[head, at, :] = chunk[tail - rows : tail, lanes]
            notes = chunk[tail : tail + TAIL, :].astype(jnp.float32)
            source = me ^ (CORES * bit + core)
            row_id = lax.broadcasted_iota(jnp.int32, (1, rows), 1) + source * rows
            key_ref[line : line + 1, :] = notes[0:1, 0:rows] * total + row_id.astype(jnp.float32)
            if core == 0:
                modes.append(notes[0:1, rows : 2 * rows])
        if direct[i].shape[0] > 3 * rows:
            for head, lanes in enumerate(heads):
                q_ref[head, i * rows : (i + 1) * rows, :] = direct[i][0:rows, lanes]
    modes += [jnp.zeros((1, rows), jnp.float32)] * (-len(modes) % 8)
    columns = key_ref[...].T
    modes = jnp.concatenate(modes, axis=0).T
    for i in range(len(bits)):
        at = slice(i * rows, (i + 1) * rows)
        line = CORES * i
        column_ref[at, :] = jnp.broadcast_to(columns[:, line : line + 1], (rows, size))
        mode = jnp.broadcast_to(modes[:, i : i + 1], (rows, size))
        for head, lanes in enumerate(heads):
            scale_ref[head, at, :] = jnp.where(
                mode == 0.0,
                gain_ref[0:1, lanes],
                jnp.where(mode == 1.0, gain_ref[1:2, lanes], gain_ref[2:3, lanes]),
            )


def attend_tiles(total, query, column_ref, k_ref, v_ref, key_ref):
    rows = key_ref.shape[1]
    chunks = k_ref.shape[0] // rows
    for first in range(0, chunks, TILE):
        last = min(first + TILE, chunks)
        keys = k_ref[first * rows : last * rows, :]
        values = v_ref[first * rows : last * rows, :]
        scores = lax.dot_general(
            query, keys, (((1,), (1,)), ((), ())), preferred_element_type=jnp.float32
        )
        weights = [
            jnp.where(
                column_ref[...] >= key_ref[i : i + 1, :],
                scores[:, (i - first) * rows : (i - first + 1) * rows],
                0.0,
            ).astype(jnp.bfloat16)
            for i in range(first, last)
        ]
        part = jnp.dot(
            jnp.concatenate(weights, axis=1), values, preferred_element_type=jnp.float32
        )
        total = part if total is None else total + part
    return total


def meet(total, head, queries, keys):
    q_ref, _, _, _, column_ref, _ = queries
    _, k_ref, v_ref, key_ref, _, _ = keys
    return attend_tiles(
        total, q_ref[head], column_ref, k_ref.at[head], v_ref.at[head], key_ref
    )


def finish(combined, gains):
    scale = lax.rsqrt(jnp.mean(combined * combined, axis=-1, keepdims=True) + 1e-06)
    normed = (combined * scale).astype(jnp.bfloat16)
    return (normed.astype(jnp.float32) * gains).astype(jnp.bfloat16)


def read_gain(gain_ref, held_ref, sem):
    columns = held_ref.shape[1]
    start = (lax.axis_index("seq") // CORES) * columns
    window = pl.ds(pl.multiple_of(start, columns), columns)
    copy = pltpu.make_async_copy(gain_ref.at[:, window], held_ref, sem)
    copy.start()
    copy.wait()


def take_up(bits, gain_ref, refs, laid):
    lay(bits, refs[: len(bits)], refs[len(bits) :], gain_ref, *laid)


def stage_kernel(olds, bits, gain_ref, *refs):
    if not olds:
        *refs, held_ref, sem = refs
        read_gain(gain_ref, held_ref, sem)
        gain_ref = held_ref
    sets = [refs[7 * i : 7 * i + 7] for i in range(olds)]
    refs = refs[7 * olds :]
    chunks, refs = refs[: 2 * len(bits)], refs[2 * len(bits) :]
    sums, new_sum, laid = refs[:olds], refs[olds], refs[olds + 1 :]
    take_up(bits, gain_ref, chunks, laid)
    for head in range(CORES):
        for out_ref, (sum_ref, *old) in zip(sums, sets):
            out_ref[head] = meet(sum_ref[head], head, old, laid)
        combined = None
        for _, *old in sets:
            combined = meet(combined, head, laid, old)
        new_sum[head] = meet(combined, head, laid, laid)


def write_back(out_refs, head, mixed):
    rows, size = out_refs[0].shape[0], mixed.shape[1]
    for i, out_ref in enumerate(out_refs):
        out_ref[:, head * size : (head + 1) * size] = mixed[i * rows : (i + 1) * rows, :]


def rest_kernel(picks, olds, bits, gain_ref, *refs):
    sets = [refs[7 * i : 7 * i + 7] for i in range(olds)]
    refs = refs[7 * olds :]
    count = sum(high - low for _, low, high in picks)
    if bits:
        chunks, refs = refs[: 2 * len(bits)], refs[2 * len(bits) :]
        outs, laid = refs[:count], refs[count:]
        take_up(bits, gain_ref, chunks, laid)
    else:
        laid, outs = refs[:6], refs[6:]
    rows = outs[0].shape[0]
    _, k_ref, v_ref, key_ref, _, _ = laid
    for place, low, high in picks:
        sum_ref, q_ref, _, _, _, column_ref, scale_ref = sets[place]
        mine, outs = outs[: high - low], outs[high - low :]
        part = slice(low * rows, high * rows)
        for head in range(CORES):
            combined = attend_tiles(
                sum_ref[head, part, :],
                q_ref[head, part, :],
                column_ref.at[part, :],
                k_ref.at[head],
                v_ref.at[head],
                key_ref,
            )
            write_back(mine, head, finish(combined, scale_ref[head, part, :]))


def new_kernel(olds, query_ref, *refs):
    laid, refs = refs[:6], refs[6:]
    sets = [refs[7 * i + 1 : 7 * i + 7] for i in range(olds)]
    outs = refs[7 * olds :]
    size = laid[1].shape[2]
    for head in range(CORES):
        query = query_ref[:, head * size : (head + 1) * size]
        combined = None
        for _, k_ref, v_ref, key_ref, _, _ in sets + [laid]:
            combined = attend_tiles(
                combined, query, laid[4], k_ref.at[head], v_ref.at[head], key_ref
            )
        write_back(outs, head, finish(combined, laid[5][head]))


def call(kernel, gain, operands, out_shapes, scratch_shapes, pairs, rows, read=False):
    held = [((gain.shape[0], CORES * HEAD_DIM), jnp.float32)] if read else []
    shapes = out_shapes + held
    scratch = [pltpu.VMEM(*shape) for shape in scratch_shapes]
    return list(
        pl.pallas_call(
            kernel,
            in_specs=[HBM if read else VMEM] + [VMEM] * len(operands),
            out_specs=[VMEM] * len(shapes),
            out_shape=[jax.ShapeDtypeStruct(*shape) for shape in shapes],
            scratch_shapes=scratch + ([pltpu.SemaphoreType.DMA(())] if read else []),
            compiler_params=pltpu.CompilerParams(vmem_limit_bytes=24 << 20),
            cost_estimate=pl.CostEstimate(
                flops=8 * CORES * rows * rows * HEAD_DIM * pairs,
                bytes_accessed=1 << 20,
                transcendentals=0,
            ),
        )(gain, *operands)
    )


def unpack_kernel(bits, *refs):
    in_refs, (*_, out_ref, sems) = refs[: len(bits)], refs[len(bits) :]
    chip = lax.axis_index("seq") // CORES
    copies = []
    for i, (bit, in_ref) in enumerate(zip(bits, in_refs)):
        width = in_ref.shape[1]
        columns = pl.ds(pl.multiple_of((chip ^ bit) * width, width), width)
        copies.append(pltpu.make_async_copy(in_ref, out_ref.at[:, columns], sems.at[i]))
    for copy in copies:
        copy.start()
    for copy in copies:
        copy.wait()


def merged(picks):
    joined = []
    for place, low, high in picks:
        if joined and joined[-1][0] == place and joined[-1][2] == low:
            joined[-1] = (place, joined[-1][1], high)
        else:
            joined.append((place, low, high))
    return joined


def plan_of(chips):
    half = chips // 2
    far = list(range(half, chips))
    near = list(range(half // 2, half)) + list(range(1, half // 2))
    send = []
    for i, bit in enumerate(far):
        send += [bit] if i == len(far) - 1 else [bit] + near[i : i + 1]
    early = far[: len(far) // 2]
    stages = [[0, near[0], early[0]], near[1:] + early[1:], far[len(early) : -1], far[-1:]]
    alike = [bit for bit in near if bit < half // 2]
    other = [bit for bit in near if bit >= half // 2]
    return send, stages, far[len(early) : -1] + early + far[-1:] + alike + other[::-1]


def by_heads(q_rows, k_rows, v_rows, block_of, modality, out_gain):
    rows = q_rows.shape[0]
    peers = lax.axis_size("seq")
    rows_in = (q_rows, k_rows, v_rows, block_of.reshape(1, rows), modality.reshape(1, rows))
    send, stages, order = plan_of(peers // CORES)

    def across(x, bit):
        return lax.ppermute(x, "seq", [(i, i ^ (CORES * bit)) for i in range(peers)])

    last = send[-1]
    jobs = [(bit, "qkv") for bit in send[:-1]] + [(last, "kv"), (last, "q")]
    sent = list(pack(jobs[:FIRST], *rows_in))
    *more, own = pack(jobs[FIRST:] + [(0, "qkv")], *rows_in)
    direct, passed = {0: own}, {}
    for (bit, parts), chunk in zip(jobs, sent + more):
        chunk = across(chunk, bit)
        if parts == "q":
            query = chunk
        else:
            direct[bit] = chunk
    for bit in [bit for bits in stages for bit in bits]:
        passed[bit] = lax.ppermute(direct[bit], "seq", [(i, i ^ 1) for i in range(peers)])
    gain = pltpu.with_memory_space_constraint(out_gain, pltpu.HBM)
    sets, taken = [], []
    for bits in stages[:-1]:
        chunks = [direct[bit] for bit in bits] + [passed[bit] for bit in bits]
        pairs = len(bits) * (2 * sum(len(one) for one in taken) + len(bits))
        laid = laid_shapes(len(bits), rows)
        shapes = [(one[0].shape, jnp.float32) for one in sets]
        shapes += [((CORES, len(bits) * rows, HEAD_DIM), jnp.float32)] + laid
        kernel = functools.partial(stage_kernel, len(sets), bits)
        operands = [x for one in sets for x in one] + chunks
        made = call(kernel, gain, operands, shapes, [], pairs, rows, not sets)
        if not sets:
            gain = made.pop()
        old = len(sets)
        sets = [[total] + one[1:] for total, one in zip(made, sets)] + [made[old:]]
        taken.append(bits)
    flat = [x for one in sets for x in one]
    piece = ((rows, CORES * HEAD_DIM), q_rows.dtype)
    half = peers // CORES // 2
    picks, owners = {True: [], False: []}, {True: [], False: []}
    for place, bits in enumerate(taken):
        for low, bit in enumerate(bits):
            picks[bit >= half].append((place, low, low + 1))
            owners[bit >= half].append(bit)
    kernel = functools.partial(rest_kernel, merged(picks[True]), len(sets), [last])
    shapes = [piece] * len(owners[True]) + laid_shapes(1, rows)
    operands = flat + [direct[last], passed[last]]
    made = call(kernel, gain, operands, shapes, [], len(owners[True]), rows)
    count = len(owners[True])
    done, laid = dict(zip(owners[True], made)), made[count:]
    kernel = functools.partial(new_kernel, len(sets))
    done[last] = call(kernel, query, laid + flat, [piece], [], peers // CORES, rows)[0]
    kernel = functools.partial(rest_kernel, merged(picks[False]), len(sets), [])
    shapes = [piece] * len(owners[False])
    made = call(kernel, gain, flat + laid, shapes, [], len(owners[False]), rows)
    done.update(zip(owners[False], made))
    for bit in order:
        done[bit] = across(done[bit], bit)
    late = order[-4:]
    out = []
    for bits in ([0] + [x for x in order if x not in late], late):
        out = [
            pl.pallas_call(
                functools.partial(unpack_kernel, bits),
                in_specs=[VMEM] * len(bits) + [HBM] * len(out),
                out_specs=HBM,
                out_shape=jax.ShapeDtypeStruct(q_rows.shape, q_rows.dtype),
                scratch_shapes=[pltpu.SemaphoreType.DMA((len(bits),))],
                input_output_aliases={len(bits): 0} if out else {},
                compiler_params=pltpu.CompilerParams(vmem_limit_bytes=8 << 20),
            )(*[done[bit] for bit in bits], *out)
        ]
    return out[0]


def fits_heads(peers, rows):
    return peers == HEADS and rows == HEAD_DIM and peers >= 16 and peers & (peers - 1) == 0


def on_device(q_rows, k_rows, v_rows, block_of, modality, out_gain):
    fits = fits_heads(lax.axis_size("seq"), q_rows.shape[0])
    plan = by_heads if fits else by_blocks
    return plan(q_rows, k_rows, v_rows, block_of, modality, out_gain)


def solution(mesh):
    placed = (
        P(("groups", "seq"), None),
        P(("groups", "seq"), None),
        P(("groups", "seq"), None),
        P(("groups", "seq"), None),
        P(("groups", "seq")),
        P(),
    )
    return jax.shard_map(
        on_device, mesh=mesh, in_specs=placed, out_specs=P(("groups", "seq"), None), check_vma=False
    )
```
